32 devices in a mesh: seq: 4 (over y, x), blk: 8 (over z, core).
Axes of the slice: x: 2, y: 2, z: 4, core: 2. Of those that a mesh axis runs over, the one named last changes fastest.
Arguments:
- queries: bfloat16 [4, 2048, 2048], P('seq', 'blk'), may hold values from -150 to 150
- keys: bfloat16 [4, 256, 2048], P('seq', 'blk'), may hold values from -6 to 6
- values: bfloat16 [4, 256, 2048], P('seq', 'blk'), may hold values from -6 to 6
- image_index: int32 [4, 2048], P('seq', 'blk'), may hold values from 0 to 3, as said below
- head_gate: float32 [16], replicated, may hold values from 0.3 to 1.5
- out_weight: bfloat16 [2048, 4096], P(None, 'blk'), may hold values from -0.125 to 0.125
Outputs:
- layer_out: bfloat16 [4, 2048, 4096], P('seq', 'blk')
The draws below stay inside these ranges and needn't reach their ends.
Inputs may be any that keep to these rules, and one draw needn't show every extreme that they name: Along each sequence image_index never falls; each image's run of text tokens is at least 256 long, so one device's tokens meet at most two images.
All inputs are finite; a program needn't handle non-finite values.
Results may differ from the reference program's by a relative error of at most 0.008.
Values may be sent and summed in bfloat16 or wider, within the bound.
No kernel may reach another device: no remote copies, remote signals or barrier semaphores. Data moves between devices by JAX's collectives and lax.ppermute only.
A program may use at most 128 MiB of HBM per device.

```python
import jax
import jax.numpy as jnp
from jax import lax

D = 4096
HEADS = 16
HD = 128
IMAGES = 4
TOK_DEV = 256
HQ = 2048
SEQS = 4
TEXT = 2048
LATENTS = 256
LAT_IMG = 64
TXT_IMG = 512


def image_layout(key):
    offsets = jax.random.randint(jax.random.fold_in(key, 11), (SEQS, IMAGES - 1), -(TXT_IMG // 4), TXT_IMG // 4 + 1)
    bounds = offsets + TXT_IMG * jnp.arange(1, IMAGES, dtype=jnp.int32)[None, :]
    positions = jnp.arange(TEXT, dtype=jnp.int32)
    return jnp.sum((positions[None, :, None] >= bounds[:, None, :]).astype(jnp.int32), axis=2)


def latent_keys(key):
    base = jax.random.truncated_normal(jax.random.fold_in(key, 22), -6.0, 6.0, (SEQS, LATENTS, HEADS * HD), jnp.float32)
    return base


def draw_keys(key, part):
    return latent_keys(key).astype(jnp.bfloat16)


def draw_queries(key, part):
    base = jax.random.truncated_normal(jax.random.fold_in(key, 33), -6.0, 6.0, (SEQS, TEXT, HEADS * HD), jnp.float32)
    return base.astype(jnp.bfloat16)


def draw_image_index(key, part):
    return image_layout(key)


def block_scale(own_key, dims, pieces, low, high):
    loudness = 1.0
    for axis_at, blocks in pieces:
        draws = jax.random.uniform(jax.random.fold_in(jax.random.fold_in(own_key, 6), axis_at), (blocks,), jnp.float32, low / len(pieces), high / len(pieces))
        loudness = loudness * jnp.repeat(jnp.exp(draws), dims[axis_at] // blocks).reshape((-1,) + (1,) * (len(dims) - 1 - axis_at))
    return loudness


def scatter_about(rng, extent, scale, bound, shards=(), held_as=jnp.bfloat16):
    drawn = scale * jax.random.normal(rng, extent, jnp.float32)
    if shards:
        drawn = drawn * block_scale(rng, extent, shards, -0.22, 0.18)
    return jnp.clip(drawn, -bound, bound).astype(held_as)


def setup_inputs(seed: int = 0) -> dict:
    arg_keys = jax.random.split(jax.random.key(seed), 7)
    queries = draw_queries(jax.random.fold_in(arg_keys[6], 71), 0)
    keys = draw_keys(jax.random.fold_in(arg_keys[6], 71), 0)
    values = scatter_about(arg_keys[2], (SEQS, LATENTS, HQ), 1.0, 6.0, ((0, 4), (1, 8)))
    image_index = draw_image_index(jax.random.fold_in(arg_keys[6], 71), 0)
    head_gate = jnp.clip(jax.random.uniform(arg_keys[4], (HEADS,), jnp.float32, 0.3, 1.5), 0.3, 1.5)
    out_weight = scatter_about(arg_keys[5], (HQ, D), HQ ** -0.5, 0.125, ((1, 8),))
    return dict(queries=queries, keys=keys, values=values, image_index=image_index, head_gate=head_gate, out_weight=out_weight)


def reference(queries, keys, values, image_index, head_gate, out_weight):
    heads = head_gate.shape[0]
    head_size = queries.shape[2] // heads
    scaling = head_size ** -0.5
    latent_image = jnp.arange(LATENTS, dtype=jnp.int32) // LAT_IMG
    gate_value = jnp.tanh(head_gate.astype(jnp.float32))

    def one_sequence(seq_args):
        query_seq, key_seq, value_seq, image_seq = seq_args
        key_heads = key_seq.astype(jnp.float32).reshape(LATENTS, heads, head_size)
        value_heads = value_seq.astype(jnp.float32).reshape(LATENTS, heads, head_size)

        def one_block(block_args):
            query_block, image_block = block_args
            query_heads = query_block.astype(jnp.float32).reshape(-1, heads, head_size)
            scores = jnp.einsum("thd,lhd->thl", query_heads, key_heads, precision=lax.Precision.HIGHEST) * scaling
            allowed = latent_image[None, None, :] <= image_block[:, None, None]
            largest = jnp.max(jnp.where(allowed, scores, -1e30), axis=2, keepdims=True)
            probs = jnp.exp(jnp.where(allowed, scores - largest, -1e30))
            denom = jnp.sum(probs, axis=2)
            rounded = lax.optimization_barrier(probs.astype(jnp.bfloat16)).astype(jnp.float32)
            weighted = jnp.einsum("thl,lhd->thd", rounded, value_heads, precision=lax.Precision.HIGHEST)
            attended = weighted / denom[:, :, None] * gate_value[None, :, None]
            hidden = attended.reshape(query_heads.shape[0], -1).astype(jnp.bfloat16)
            return jnp.dot(hidden, out_weight, preferred_element_type=jnp.float32).astype(jnp.bfloat16)

        blocks = lax.map(one_block, (query_seq.reshape(TEXT // TOK_DEV, TOK_DEV, -1),
                                     image_seq.reshape(TEXT // TOK_DEV, TOK_DEV)))
        return blocks.reshape(TEXT, -1)

    return lax.map(one_sequence, (queries, keys, values, image_index))
```

```python
import functools

import jax
import jax.numpy as jnp
from jax import lax
from jax.experimental import pallas as pl
from jax.experimental.pallas import tpu as pltpu
from jax.sharding import PartitionSpec as P

IMAGES = 4


def attend_kernel(heads, latents, packed, gate_ref, images_ref, latent_image_ref, q_ref, *refs):
    blocks, (out_ref, key_all, value_all) = refs[:-3], refs[-3:]
    at = 0
    for i, together in enumerate(packed):
        rows = slice(i * latents, (i + 1) * latents)
        if together:
            key_all[rows, :] = blocks[at][:latents, :]
            value_all[rows, :] = blocks[at][latents:, :]
            at += 1
        else:
            key_all[rows, :] = blocks[at][...]
            value_all[rows, :] = blocks[at + 1][...]
            at += 2
    size = q_ref.shape[1] // heads
    allowed = latent_image_ref[...] <= images_ref[...]
    for h in range(heads):
        lanes = slice(h * size, (h + 1) * size)
        scores = lax.dot_general(
            q_ref[:, lanes], key_all[:, lanes], (((1,), (1,)), ((), ())), preferred_element_type=jnp.float32
        ) * size ** (-0.5)
        scores = jnp.where(allowed, scores, -1e30)
        probs = jnp.where(allowed, jnp.exp(scores - jnp.max(scores, axis=1, keepdims=True)), 0.0)
        denom = jnp.sum(probs, axis=1, keepdims=True)
        weighted = jnp.dot(probs.astype(jnp.bfloat16), value_all[:, lanes], preferred_element_type=jnp.float32)
        out_ref[:, lanes] = (weighted / denom * gate_ref[:, h : h + 1]).astype(jnp.bfloat16)


def project_kernel(hidden_ref, *refs):
    units, (own_ref, other_ref) = refs[:-2], refs[-2:]
    total, at = None, 0
    for unit in units:
        rows = unit.shape[0]
        part = jnp.dot(hidden_ref[:, at : at + rows], unit[...], preferred_element_type=jnp.float32)
        total = part if total is None else total + part
        at += rows
    tokens = own_ref.shape[0]
    own_ref[...] = total[:tokens].astype(jnp.bfloat16)
    other_ref[...] = total[tokens:].astype(jnp.bfloat16)


def project(hidden, units):
    tokens, cols = hidden.shape[0] // 2, units[0].shape[1]
    shape = jax.ShapeDtypeStruct((tokens, cols), jnp.bfloat16)
    flops = 2 * hidden.shape[0] * hidden.shape[1] * cols
    return pl.pallas_call(
        project_kernel,
        out_shape=(shape, shape),
        cost_estimate=pl.CostEstimate(flops=flops, transcendentals=0, bytes_accessed=hidden.size * 2),
        name="project",
    )(hidden, *units)


def place_kernel(count, where_ref, *refs):
    mine, theirs, out_ref = refs[:count], refs[count : 2 * count], refs[2 * count]
    cols = mine[0].shape[1]
    step = pl.program_id(0)
    core = where_ref[1]
    for i in range(count):

        @pl.when((step == i) & (core == 0))
        def _():
            out_ref[:, :cols] = mine[i][...]
            out_ref[:, cols:] = theirs[i][...]

        @pl.when((step == i) & (core == 1))
        def _():
            out_ref[:, :cols] = theirs[i][...]
            out_ref[:, cols:] = mine[i][...]


def place(where, mine, theirs):
    count = len(mine)
    tokens, cols = mine[0].shape
    whole = pl.BlockSpec((tokens, cols), lambda i, where: (0, 0))
    return pl.pallas_call(
        functools.partial(place_kernel, count),
        grid_spec=pltpu.PrefetchScalarGridSpec(
            num_scalar_prefetch=1,
            grid=(count,),
            in_specs=[whole] * (2 * count),
            out_specs=pl.BlockSpec((tokens, 2 * cols), lambda i, where: (0, lax.rem(where[0] + i, count))),
        ),
        out_shape=jax.ShapeDtypeStruct((tokens, 2 * cols * count), jnp.bfloat16),
        name="place",
    )(where, *mine, *theirs)


def per_device(queries, keys, values, image_index, head_gate, out_weight):
    blocks, seqs = lax.axis_size("blk"), lax.axis_size("seq")
    chips = blocks // 2
    me, seq = lax.axis_index("blk"), lax.axis_index("seq")
    chip, core = me // 2, me % 2
    parity = (seq ^ (seq >> 1)) & 1
    heads = head_gate.shape[0]
    tokens, width = queries.shape[1:]
    latents = keys.shape[1]

    def up(x):
        return lax.ppermute(x, "blk", [(i, (i + 2) % blocks) for i in range(blocks)])

    def down(x):
        return lax.ppermute(x, "blk", [(i, (i - 2) % blocks) for i in range(blocks)])

    def across(x):
        return lax.ppermute(x, "blk", [(i, i ^ 1) for i in range(blocks)])

    def first_side(x):
        return lax.ppermute(x, "seq", [(i, i ^ 1) for i in range(seqs)])

    def second_side(x):
        return lax.ppermute(x, "seq", [(i, i ^ 2) for i in range(seqs)])

    half = out_weight.shape[0] // 2
    quarter = half // 2
    cols = out_weight.shape[1]
    a = lax.dynamic_slice(out_weight, (parity * half, 0), (quarter, cols))
    b = lax.dynamic_slice(out_weight, (parity * half + quarter, 0), (quarter, cols))

    pieces, latent_blocks = {}, {0: (jnp.concatenate([keys[0], values[0]], axis=0),)}
    up_kv = down_kv = latent_blocks[0][0]
    up_a = down_a = a
    up_b = down_b = b
    for k in range(1, chips // 2 + 1):
        if 2 * k == chips:
            up_a, down_b = up(up_a), down(down_b)
            pieces[k] = (up_a, down_b)
            latent_blocks[k] = (up(up_kv[:latents]), down(down_kv[latents:]))
        else:
            up_a, down_b = up(up_a), down(down_b)
            up_kv, down_kv = up(up_kv), down(down_kv)
            up_b, down_a = up(up_b), down(down_a)
            pieces[chips - k], pieces[k] = (up_a, up_b), (down_a, down_b)
            latent_blocks[chips - k], latent_blocks[k] = (up_kv,), (down_kv,)

    packed, arrays, first_rows = [], [], []
    for d in latent_blocks:
        for side in range(2):
            packed.append(len(latent_blocks[d]) == 1)
            arrays += [across(x) if side else x for x in latent_blocks[d]]
            first_rows.append((lax.rem(chip + d, chips) * 2 + (core ^ side)) * latents)
    latent = (jnp.stack(first_rows)[:, None] + lax.iota(jnp.int32, latents)[None, :]).reshape(1, -1)
    latent_image = latent // (latents * blocks // IMAGES)

    hidden = pl.pallas_call(
        functools.partial(attend_kernel, heads, latents, tuple(packed)),
        out_shape=jax.ShapeDtypeStruct((tokens, width), jnp.bfloat16),
        scratch_shapes=[pltpu.VMEM((latents * blocks, width), jnp.bfloat16)] * 2,
        cost_estimate=pl.CostEstimate(
            flops=4 * tokens * latents * blocks * width * 4, transcendentals=0, bytes_accessed=tokens * width * 4
        ),
        name="attend",
    )(jnp.tanh(head_gate)[None], image_index[0][:, None], latent_image, queries[0], *arrays)

    both = jnp.concatenate([hidden, across(hidden)], axis=0)
    rolled = jnp.where(parity == 0, both, jnp.concatenate([both[:, half:], both[:, :half]], axis=1))

    mine, theirs = [None] * chips, [None] * chips
    order = [0] + sorted(pieces, key=lambda d: min(d, chips - d))
    for d in order:
        if d == 0:
            own, other = project(both, [out_weight])
        else:
            first, second = pieces[d]
            own, other = project(rolled, [first, second, first_side(first), second_side(second)])
        mine[d], theirs[d] = own, across(other)
    return place(jnp.stack([chip, core]).astype(jnp.int32), mine, theirs)[None]


def solution(mesh):
    placed = (
        P("seq", "blk", None),
        P("seq", "blk", None),
        P("seq", "blk", None),
        P("seq", "blk"),
        P(),
        P(None, "blk"),
    )
    return jax.shard_map(
        per_device, mesh=mesh, in_specs=placed, out_specs=P("seq", "blk", None), check_vma=False
    )
```

```python
import functools

import jax
import jax.numpy as jnp
from jax import lax
from jax.experimental import pallas as pl
from jax.experimental.pallas import tpu as pltpu
from jax.sharding import PartitionSpec as P


IMAGES = 4


def attend_kernel(heads, latents, packed, gate_ref, images_ref, latent_image_ref, q_ref, *refs):
    blocks, (out_ref, key_all, value_all) = refs[:-3], refs[-3:]
    at = 0
    for i, together in enumerate(packed):
        rows = slice(i * latents, (i + 1) * latents)
        if together:
            key_all[rows, :] = blocks[at][:latents, :]
            value_all[rows, :] = blocks[at][latents:, :]
            at += 1
        else:
            key_all[rows, :] = blocks[at][...]
            value_all[rows, :] = blocks[at + 1][...]
            at += 2
    size = q_ref.shape[1] // heads
    allowed = latent_image_ref[...] <= images_ref[...]
    for h in range(heads):
        lanes = slice(h * size, (h + 1) * size)
        scores = lax.dot_general(
            q_ref[:, lanes], key_all[:, lanes], (((1,), (1,)), ((), ())), preferred_element_type=jnp.float32
        ) * size ** (-0.5)
        scores = jnp.where(allowed, scores, -1e30)
        probs = jnp.where(allowed, jnp.exp(scores - jnp.max(scores, axis=1, keepdims=True)), 0.0)
        denom = jnp.sum(probs, axis=1, keepdims=True)
        weighted = jnp.dot(probs.astype(jnp.bfloat16), value_all[:, lanes], preferred_element_type=jnp.float32)
        out_ref[:, lanes] = (weighted / denom * gate_ref[:, h : h + 1]).astype(jnp.bfloat16)


def project_kernel(hidden_ref, *refs):
    units, (own_ref, other_ref) = refs[:-2], refs[-2:]
    total, at = None, 0
    for unit in units:
        rows = unit.shape[0]
        part = jnp.dot(hidden_ref[:, at : at + rows], unit[...], preferred_element_type=jnp.float32)
        total = part if total is None else total + part
        at += rows
    tokens = own_ref.shape[0]
    own_ref[...] = total[:tokens].astype(jnp.bfloat16)
    other_ref[...] = total[tokens:].astype(jnp.bfloat16)


def project(hidden, units):
    tokens, cols = hidden.shape[0] // 2, units[0].shape[1]
    shape = jax.ShapeDtypeStruct((tokens, cols), jnp.bfloat16)
    flops = 2 * hidden.shape[0] * hidden.shape[1] * cols
    return pl.pallas_call(
        project_kernel,
        out_shape=(shape, shape),
        cost_estimate=pl.CostEstimate(flops=flops, transcendentals=0, bytes_accessed=hidden.size * 2),
        name="project",
    )(hidden, *units)


def place_kernel(count, where_ref, *refs):
    mine, theirs, out_ref = refs[:count], refs[count : 2 * count], refs[-1]
    cols = mine[0].shape[1]
    step = pl.program_id(0)
    core = where_ref[0]
    for i in range(count):

        @pl.when((step == i) & (core == 0))
        def _():
            out_ref[:, :cols] = mine[i][...]
            out_ref[:, cols:] = theirs[i][...]

        @pl.when((step == i) & (core == 1))
        def _():
            out_ref[:, :cols] = theirs[i][...]
            out_ref[:, cols:] = mine[i][...]


def place(core, at, mine, theirs, chips, out=None):
    count = len(mine)
    tokens, cols = mine[0].shape
    whole = pl.BlockSpec((tokens, cols), lambda i, where: (0, 0))
    before = () if out is None else (out,)
    return pl.pallas_call(
        functools.partial(place_kernel, count),
        grid_spec=pltpu.PrefetchScalarGridSpec(
            num_scalar_prefetch=1,
            grid=(count,),
            in_specs=[whole] * (2 * count) + [pl.BlockSpec(memory_space=pl.ANY)] * len(before),
            out_specs=pl.BlockSpec((tokens, 2 * cols), lambda i, where: (0, where[1 + i])),
        ),
        out_shape=jax.ShapeDtypeStruct((tokens, 2 * cols * chips), jnp.bfloat16),
        input_output_aliases={1 + 2 * count: 0} if before else {},
        name="place",
    )(jnp.stack([core, *at]).astype(jnp.int32), *mine, *theirs, *before)


def steps(chips):
    far = chips // 2
    order = [("kv_up", 1), ("kv_down", 1), ("a_up", 1), ("b_down", 1), ("kv_swap", 0)]
    for k in range(2, far + 1):
        order += [("kv_up", k), ("kv_down", k), ("a_down", k - 1), ("b_up", k - 1)]
        order += [("kv_swap_up", k - 1), ("kv_swap_down", k - 1), ("x_up", k - 1), ("y_down", k - 1)]
        order += [("a_up", k), ("b_down", k)]
        if k > 2:
            order += [("x_down", k - 2), ("y_up", k - 2)]
    order += [("kv_swap_up", far), ("kv_swap_down", far), ("attend", 0), ("hidden_swap", 0)]
    if far > 1:
        order += [("x_down", far - 1), ("y_up", far - 1)]
    order += [("project", 0), ("x_up", far), ("y_down", far)]
    for k in range(1, far):
        order += [("project_up", k), ("project_down", k)]
    return order + [("place", 0), ("project", far), ("place", 1)]


def per_device(queries, keys, values, image_index, head_gate, out_weight):
    blocks, seqs = lax.axis_size("blk"), lax.axis_size("seq")
    chips = blocks // 2
    far = chips // 2
    me, seq = lax.axis_index("blk"), lax.axis_index("seq")
    chip, core = me // 2, me % 2
    parity = (seq ^ (seq >> 1)) & 1
    heads = head_gate.shape[0]
    tokens, width = queries.shape[1:]
    latents = keys.shape[1]

    half = out_weight.shape[0] // 2
    quarter = half // 2
    cols = out_weight.shape[1]
    kv = jnp.concatenate([keys[0], values[0]], axis=0)
    a = lax.dynamic_slice(out_weight, (parity * half, 0), (quarter, cols))
    b = lax.dynamic_slice(out_weight, (parity * half + quarter, 0), (quarter, cols))

    moved = {("kv_up", 0): kv, ("kv_down", 0): kv}
    for name in ("a_up", "a_down"):
        moved[name, 0] = a
    for name in ("b_up", "b_down"):
        moved[name, 0] = b

    def shift(x, by):
        return lax.ppermute(x, "blk", [(i, (i + 2 * by) % blocks) for i in range(blocks)])

    def swap(x):
        return lax.ppermute(x, "blk", [(i, i ^ 1) for i in range(blocks)])

    def side(x, bit):
        return lax.ppermute(x, "seq", [(i, i ^ bit) for i in range(seqs)])

    def attend():
        packed, arrays, first_rows = [], [], []
        for k in range(far + 1):
            for name, d in (("up", -k), ("down", k)) if 0 < k < far else (("", k),):
                for other in range(2):
                    if k == 0:
                        found = [moved["kv_swap", 0] if other else kv]
                    elif k < far:
                        found = [moved[f"kv_swap_{name}" if other else f"kv_{name}", k]]
                    else:
                        found = [moved[f"kv_swap_{n}" if other else f"kv_{n}", k] for n in ("up", "down")]
                    packed.append(len(found) == 1)
                    arrays += found
                    first_rows.append((lax.rem(chip + d + chips, chips) * 2 + (core ^ other)) * latents)
        latent = (jnp.stack(first_rows)[:, None] + lax.iota(jnp.int32, latents)[None, :]).reshape(1, -1)
        latent_image = latent // (latents * blocks // IMAGES)
        return pl.pallas_call(
            functools.partial(attend_kernel, heads, latents, tuple(packed)),
            out_shape=jax.ShapeDtypeStruct((tokens, width), jnp.bfloat16),
            scratch_shapes=[pltpu.VMEM((latents * blocks, width), jnp.bfloat16)] * 2,
            name="attend",
        )(jnp.tanh(head_gate)[None], image_index[0][:, None], latent_image, queries[0], *arrays)

    def units(k, name):
        first = moved["a_up" if name != "down" else "a_down", k]
        second = moved["b_down" if name != "up" else "b_up", k]
        return [first, second, moved["x_down" if name == "down" else "x_up", k], moved["y_up" if name == "up" else "y_down", k]]

    mine, theirs, at = [], [], []
    out = None
    hidden = both = rolled = None
    for name, k in steps(chips):
        if name in ("kv_up", "kv_down") and k == far:
            before = moved[name, k - 1]
            moved[name, k] = shift(before[:latents] if name == "kv_up" else before[latents:], 1 if name == "kv_up" else -1)
        elif name in ("kv_up", "a_up", "b_up"):
            moved[name, k] = shift(moved[name, k - 1], 1)
        elif name in ("kv_down", "a_down", "b_down"):
            moved[name, k] = shift(moved[name, k - 1], -1)
        elif name == "kv_swap":
            moved[name, k] = swap(kv)
        elif name in ("kv_swap_up", "kv_swap_down"):
            moved[name, k] = swap(moved[name.replace("swap_", ""), k])
        elif name in ("x_up", "x_down"):
            moved[name, k] = side(moved[name.replace("x", "a"), k], 1)
        elif name in ("y_up", "y_down"):
            moved[name, k] = side(moved[name.replace("y", "b"), k], 2)
        elif name == "attend":
            hidden = attend()
        elif name == "hidden_swap":
            both = jnp.concatenate([hidden, swap(hidden)], axis=0)
            rolled = jnp.where(parity == 0, both, jnp.concatenate([both[:, half:], both[:, :half]], axis=1))
        elif name == "place":
            out = place(core, at, mine, theirs, chips, out)
            mine, theirs, at = [], [], []
        else:
            which = name[len("project_") :]
            own, other = project(both, [out_weight]) if k == 0 else project(rolled, units(k, which))
            mine.append(own)
            theirs.append(swap(other))
            at.append(lax.rem(chip + chips + (-k if which == "up" else k), chips))
    return out[None]


def solution(mesh):
    placed = (
        P("seq", "blk", None),
        P("seq", "blk", None),
        P("seq", "blk", None),
        P("seq", "blk"),
        P(),
        P(None, "blk"),
    )

    return jax.shard_map(per_device, mesh=mesh, in_specs=placed, out_specs=P("seq", "blk", None), check_vma=False)
```

```python
import functools

import jax
import jax.numpy as jnp
from jax import lax
from jax.experimental import pallas as pl
from jax.experimental.pallas import tpu as pltpu
from jax.sharding import PartitionSpec as P


IMAGES = 4


def attend_kernel(heads, latents, packed, gate_ref, images_ref, latent_image_ref, q_ref, *refs):
    blocks, (out_ref, key_all, value_all) = refs[:-3], refs[-3:]
    at = 0
    for i, together in enumerate(packed):
        rows = slice(i * latents, (i + 1) * latents)
        if together:
            key_all[rows, :] = blocks[at][:latents, :]
            value_all[rows, :] = blocks[at][latents:, :]
            at += 1
        else:
            key_all[rows, :] = blocks[at][...]
            value_all[rows, :] = blocks[at + 1][...]
            at += 2
    size = q_ref.shape[1] // heads
    allowed = latent_image_ref[...] <= images_ref[...]
    for h in range(heads):
        lanes = slice(h * size, (h + 1) * size)
        scores = lax.dot_general(
            q_ref[:, lanes], key_all[:, lanes], (((1,), (1,)), ((), ())), preferred_element_type=jnp.float32
        ) * size ** (-0.5)
        scores = jnp.where(allowed, scores, -1e30)
        probs = jnp.where(allowed, jnp.exp(scores - jnp.max(scores, axis=1, keepdims=True)), 0.0)
        denom = jnp.sum(probs, axis=1, keepdims=True)
        weighted = jnp.dot(probs.astype(jnp.bfloat16), value_all[:, lanes], preferred_element_type=jnp.float32)
        out_ref[:, lanes] = (weighted / denom * gate_ref[:, h : h + 1]).astype(jnp.bfloat16)


def project_kernel(hidden_ref, *refs):
    units, (own_ref, other_ref) = refs[:-2], refs[-2:]
    total, at = None, 0
    for unit in units:
        rows = unit.shape[0]
        part = jnp.dot(hidden_ref[:, at : at + rows], unit[...], preferred_element_type=jnp.float32)
        total = part if total is None else total + part
        at += rows
    tokens = own_ref.shape[0]
    own_ref[...] = total[:tokens].astype(jnp.bfloat16)
    other_ref[...] = total[tokens:].astype(jnp.bfloat16)


def project(hidden, units):
    tokens, cols = hidden.shape[0] // 2, units[0].shape[1]
    shape = jax.ShapeDtypeStruct((tokens, cols), jnp.bfloat16)
    flops = 2 * hidden.shape[0] * hidden.shape[1] * cols
    return pl.pallas_call(
        project_kernel,
        out_shape=(shape, shape),
        cost_estimate=pl.CostEstimate(flops=flops, transcendentals=0, bytes_accessed=hidden.size * 2),
        name="project",
    )(hidden, *units)


def place_kernel(count, where_ref, *refs):
    mine, theirs, out_ref = refs[:count], refs[count : 2 * count], refs[-1]
    cols = mine[0].shape[1]
    step = pl.program_id(0)
    core = where_ref[0]
    for i in range(count):

        @pl.when((step == i) & (core == 0))
        def _():
            out_ref[:, :cols] = mine[i][...]
            out_ref[:, cols:] = theirs[i][...]

        @pl.when((step == i) & (core == 1))
        def _():
            out_ref[:, :cols] = theirs[i][...]
            out_ref[:, cols:] = mine[i][...]


def place(core, at, mine, theirs, chips, out=None):
    count = len(mine)
    tokens, cols = mine[0].shape
    whole = pl.BlockSpec((tokens, cols), lambda i, where: (0, 0))
    before = () if out is None else (out,)
    return pl.pallas_call(
        functools.partial(place_kernel, count),
        grid_spec=pltpu.PrefetchScalarGridSpec(
            num_scalar_prefetch=1,
            grid=(count,),
            in_specs=[whole] * (2 * count) + [pl.BlockSpec(memory_space=pl.ANY)] * len(before),
            out_specs=pl.BlockSpec((tokens, 2 * cols), lambda i, where: (0, where[1 + i])),
        ),
        out_shape=jax.ShapeDtypeStruct((tokens, 2 * cols * chips), jnp.bfloat16),
        input_output_aliases={1 + 2 * count: 0} if before else {},
        name="place",
    )(jnp.stack([core, *at]).astype(jnp.int32), *mine, *theirs, *before)


def steps(chips):
    far = chips // 2
    order = [("kv_up", 1), ("kv_down", 1)]
    if far > 1:
        order += [("w_up", 1), ("w_down", 1)]
    order += [("kv_swap", 0)]
    for k in range(2, far + 1):
        order += [("kv_up", k), ("kv_down", k), ("kv_swap_up", k - 1), ("kv_swap_down", k - 1)]
        order += [("w_up" if k < far else "a_up", k), ("x_up", k - 1), ("y_up", k - 1)]
        order += [("w_down" if k < far else "b_down", k), ("x_down", k - 1), ("y_down", k - 1)]
        if k > 2:
            order += [("xy_up", k - 2), ("yx_up", k - 2), ("xy_down", k - 2), ("yx_down", k - 2)]
    if far == 1:
        order += [("a_up", far), ("b_down", far)]
    order += [("kv_swap_up", far), ("kv_swap_down", far), ("attend", 0), ("hidden_swap", 0)]
    if far > 1:
        order += [("xy_up", far - 1), ("yx_up", far - 1), ("xy_down", far - 1), ("yx_down", far - 1)]
    order += [("project", 0), ("xa", far), ("ya", far), ("yb", far), ("xb", far)]
    for k in range(1, far):
        order += [("project_up", k), ("project_down", k)]
    order += [("xya", far), ("yxb", far)]
    return order + [("place", 0), ("project", far), ("place", 1)]


def per_device(queries, keys, values, image_index, head_gate, out_weight):
    blocks, seqs = lax.axis_size("blk"), lax.axis_size("seq")
    chips = blocks // 2
    far = chips // 2
    me, seq = lax.axis_index("blk"), lax.axis_index("seq")
    chip, core = me // 2, me % 2
    part = seq & 3
    heads = head_gate.shape[0]
    tokens, width = queries.shape[1:]
    latents = keys.shape[1]

    quarter = out_weight.shape[0] // 4
    eighth = quarter // 2
    kv = jnp.concatenate([keys[0], values[0]], axis=0)
    w = lax.dynamic_slice(out_weight, (part * quarter, 0), (quarter, out_weight.shape[1]))
    moved = {("kv_up", 0): kv, ("kv_down", 0): kv, ("w_up", 0): w, ("w_down", 0): w}

    def shift(x, by):
        return lax.ppermute(x, "blk", [(i, (i + 2 * by) % blocks) for i in range(blocks)])

    def swap(x):
        return lax.ppermute(x, "blk", [(i, i ^ 1) for i in range(blocks)])

    def side(x, bit):
        return lax.ppermute(x, "seq", [(i, i ^ bit) for i in range(seqs)])

    def attend():
        packed, arrays, first_rows = [], [], []
        for k in range(far + 1):
            for name, d in (("up", -k), ("down", k)) if 0 < k < far else (("", k),):
                for other in range(2):
                    if k == 0:
                        found = [moved["kv_swap", 0] if other else kv]
                    elif k < far:
                        found = [moved[f"kv_swap_{name}" if other else f"kv_{name}", k]]
                    else:
                        found = [moved[f"kv_swap_{n}" if other else f"kv_{n}", k] for n in ("up", "down")]
                    packed.append(len(found) == 1)
                    arrays += found
                    first_rows.append((lax.rem(chip + d + chips, chips) * 2 + (core ^ other)) * latents)
        latent = (jnp.stack(first_rows)[:, None] + lax.iota(jnp.int32, latents)[None, :]).reshape(1, -1)
        latent_image = latent // (latents * blocks // IMAGES)
        return pl.pallas_call(
            functools.partial(attend_kernel, heads, latents, tuple(packed)),
            out_shape=jax.ShapeDtypeStruct((tokens, width), jnp.bfloat16),
            scratch_shapes=[pltpu.VMEM((latents * blocks, width), jnp.bfloat16)] * 2,
            name="attend",
        )(jnp.tanh(head_gate)[None], image_index[0][:, None], latent_image, queries[0], *arrays)

    def units(k, name):
        names = ["w_up", "x_up", "y_up", "xy_up", "yx_up"]
        if name == "down":
            names = ["w_down", "x_down", "y_down", "xy_down", "yx_down"]
        elif name != "up":
            names = ["a_up", "b_down", "xa", "xb", "ya", "yb", "xya", "yxb"]
        return [moved[n, k] for n in names]

    mine, theirs, at = [], [], []
    out = None
    hidden = both = rolled = None
    for name, k in steps(chips):
        if name in ("kv_up", "kv_down") and k == far:
            before = moved[name, k - 1]
            moved[name, k] = shift(before[:latents] if name == "kv_up" else before[latents:], 1 if name == "kv_up" else -1)
        elif name == "a_up":
            moved[name, k] = shift(moved["w_up", k - 1][:eighth], 1)
        elif name == "b_down":
            moved[name, k] = shift(moved["w_down", k - 1][eighth:], -1)
        elif name in ("kv_up", "w_up"):
            moved[name, k] = shift(moved[name, k - 1], 1)
        elif name in ("kv_down", "w_down"):
            moved[name, k] = shift(moved[name, k - 1], -1)
        elif name == "kv_swap":
            moved[name, k] = swap(kv)
        elif name in ("kv_swap_up", "kv_swap_down"):
            moved[name, k] = swap(moved[name.replace("swap_", ""), k])
        elif name in ("x_up", "x_down"):
            moved[name, k] = side(moved[name.replace("x", "w"), k], 1)
        elif name in ("y_up", "y_down"):
            moved[name, k] = side(moved[name.replace("y", "w"), k], 2)
        elif name in ("xy_up", "xy_down"):
            moved[name, k] = side(moved[name.replace("xy", "x"), k][:eighth], 2)
        elif name in ("yx_up", "yx_down"):
            moved[name, k] = side(moved[name.replace("yx", "y"), k][eighth:], 1)
        elif name in ("xa", "ya", "xb", "yb"):
            moved[name, k] = side(moved["a_up" if "a" in name else "b_down", k], 1 if "x" in name else 2)
        elif name == "xya":
            moved[name, k] = side(moved["xa", k], 2)
        elif name == "yxb":
            moved[name, k] = side(moved["yb", k], 1)
        elif name == "attend":
            hidden = attend()
        elif name == "hidden_swap":
            both = jnp.concatenate([hidden, swap(hidden)], axis=0)
            quarters = [
                lax.dynamic_slice(both, (0, (part ^ r) * quarter), (2 * tokens, quarter)) for r in range(4)
            ]
            rolled = jnp.concatenate(quarters, axis=1)
        elif name == "place":
            out = place(core, at, mine, theirs, chips, out)
            mine, theirs, at = [], [], []
        else:
            which = name[len("project_") :]
            own, other = project(both, [out_weight]) if k == 0 else project(rolled, units(k, which))
            mine.append(own)
            theirs.append(swap(other))
            at.append(lax.rem(chip + chips + (-k if which == "up" else k), chips))
    return out[None]


def solution(mesh):
    placed = (
        P("seq", "blk", None),
        P("seq", "blk", None),
        P("seq", "blk", None),
        P("seq", "blk"),
        P(),
        P(None, "blk"),
    )

    return jax.shard_map(per_device, mesh=mesh, in_specs=placed, out_specs=P("seq", "blk", None), check_vma=False)
```
